128 devices in a mesh: row: 8 (over y, core), col: 16 (over z, x).
Axes of the slice: x: 4, y: 4, z: 4, core: 2. Of those that a mesh axis runs over, the one named last changes fastest.
Arguments:
- current_left: bfloat16 [8, 256, 768, 128], P('row', 'col'), may hold values from -6 to 6
- current_right: bfloat16 [8, 256, 768, 128], P('row', 'col'), may hold values from -0.21875 to 0.21875
- current_rank: int32 [8, 256], P('row', 'col'), may hold values from 1 to 128
- target_rank: int32 [8, 256], P('row', 'col'), may hold values from 1 to 128
- update_left: bfloat16 [8, 128, 768, 128], P('row', 'col'), may hold values from -6 to 6
- update_right: bfloat16 [8, 128, 768, 128], P('row', 'col'), may hold values from -0.21875 to 0.21875
- update_rank: int32 [8, 128], P('row', 'col'), may hold values from 1 to 128
- owner_slot: int32 [8, 128], P('row', 'col'), may hold values from 0 to 255, as said below
Outputs:
- compressed_left: bfloat16 [8, 256, 768, 128], P('row', 'col')
- returned_right: bfloat16 [8, 128, 768, 128], P('row', 'col')
- row_scale: float32 [16, 768], P('row')
The draws below stay inside these ranges and needn't reach their ends.
Inputs may be any that keep to these rules, and one draw needn't show every extreme that they name: `owner_slot`: an entry is the tile's owning column index times 16 plus the tile's place on that owner. No tile is named by two contributions of its grid row. One device names either none or exactly 2 tiles of each owner. In every grid row some owner has all of its 16 tiles named.
All inputs are finite; a program needn't handle non-finite values.
Results may differ from the reference program's by a relative error of at most 0.0085.
Values may be sent and summed in bfloat16 or wider, within the bound.
No kernel may reach another device: no remote copies, remote signals or barrier semaphores. Data moves between devices by JAX's collectives and lax.ppermute only.
A program may use at most 128 MiB of HBM per device.

```python
import math
import jax
import jax.numpy as jnp
from jax import lax

TILE = 768
HALF = 128
BR = 2
SWEEPS = 8
ROOTS = 3
SLOTS = 8
TILES_ROW = 256
CONTRIB_ROW = 128
N_ROW = 8
N_COL = 16


def owner_row(row_key):
    window_order = jax.random.permutation(jax.random.fold_in(row_key, 1), N_COL)
    swing_amount = jax.random.randint(jax.random.fold_in(row_key, 2), (N_COL // 2,), 0, SLOTS // 2 + 1)
    swing_amount = swing_amount.at[0].set(SLOTS // 2)
    pair_count = jnp.stack([SLOTS // 2 + swing_amount, SLOTS // 2 - swing_amount], axis=1).reshape(N_COL)
    window_start = jnp.cumsum(pair_count) - pair_count
    perm_keys = jax.random.split(jax.random.fold_in(row_key, 3), N_COL)
    tile_perms = jax.vmap(lambda one_key: jax.random.permutation(one_key, 2 * SLOTS))(perm_keys)
    tile_place = tile_perms.reshape(N_COL, SLOTS, 2)
    pair_index = jnp.arange(SLOTS)[None, :, None]
    is_valid = jnp.broadcast_to(pair_index < pair_count[:, None, None], (N_COL, SLOTS, 2))
    source = jnp.broadcast_to((window_start[:, None, None] + pair_index) % N_COL, (N_COL, SLOTS, 2))
    owner_col = jnp.broadcast_to(window_order[:, None, None], (N_COL, SLOTS, 2))
    slot_value = (owner_col * (2 * SLOTS) + tile_place).reshape(-1)
    entry_count = N_COL * SLOTS * 2
    flat_index = jnp.arange(entry_count)
    jitter = jax.random.randint(jax.random.fold_in(row_key, 4), (entry_count,), 0, 4096)
    score = jnp.where(is_valid.reshape(-1), source.reshape(-1) * (4096 * entry_count) + jitter * entry_count + flat_index, N_COL * 4096 * entry_count + flat_index)
    picked = jnp.argsort(score, stable=True)[:N_COL * SLOTS]
    return slot_value[picked].astype(jnp.int32)


def draw_owner_slot(key, part):
    row_keys = jax.random.split(jax.random.fold_in(key, 11), N_ROW)
    return jax.vmap(owner_row)(row_keys)


def set_ends(result, key, least, largest):
    spot = [jax.random.randint(jax.random.fold_in(key, axis), (), 0, length) for axis, length in enumerate(result.shape)]
    widest = result.shape.index(max(result.shape))
    neighbour = spot[:widest] + [(spot[widest] + 1) % result.shape[widest]] + spot[widest + 1:]
    return result.at[tuple(spot)].set(least).at[tuple(neighbour)].set(largest)


def shard_levels(own_key, dims, cuts, low, high):
    def one(axis_at, blocks):
        heights = jax.random.uniform(jax.random.fold_in(jax.random.fold_in(own_key, 6), axis_at), (blocks,), jnp.float32, low / len(cuts), high / len(cuts))
        return jnp.repeat(jnp.exp(heights), dims[axis_at] // blocks).reshape((-1,) + (1,) * (len(dims) - axis_at - 1))

    factor_of = one(*cuts[0])
    for cut in cuts[1:]:
        factor_of = factor_of * one(*cut)
    return factor_of


def normal_values(own_key, dims, spread, most, pieces=(), kind=jnp.bfloat16):
    values = jax.random.normal(own_key, dims, jnp.float32) * spread
    if len(pieces) > 0:
        values = shard_levels(own_key, dims, pieces, -0.22, 0.18) * values
    return jnp.clip(values, min=-most, max=most).astype(kind)


def setup_inputs(seed: int = 0) -> dict:
    streams_of = jax.random.split(jax.random.key(seed), 9)
    return {
        "current_left": normal_values(streams_of[0], (N_ROW, TILES_ROW, TILE, HALF), 1.0, 6.0, ((0, 8), (1, 16))),
        "current_right": normal_values(streams_of[1], (N_ROW, TILES_ROW, TILE, HALF), TILE ** -0.5, 0.21875, ((0, 8), (1, 16))),
        "current_rank": set_ends(jax.random.randint(streams_of[2], (N_ROW, TILES_ROW), 1, HALF + 1), jax.random.fold_in(streams_of[2], 1), 1, HALF).astype(jnp.int32),
        "target_rank": set_ends(jax.random.randint(streams_of[3], (N_ROW, TILES_ROW), 1, HALF + 1), jax.random.fold_in(streams_of[3], 1), 1, HALF).astype(jnp.int32),
        "update_left": normal_values(streams_of[4], (N_ROW, CONTRIB_ROW, TILE, HALF), 1.0, 6.0, ((0, 8), (1, 16))),
        "update_right": normal_values(streams_of[5], (N_ROW, CONTRIB_ROW, TILE, HALF), TILE ** -0.5, 0.21875, ((0, 8), (1, 16))),
        "update_rank": set_ends(jax.random.randint(streams_of[6], (N_ROW, CONTRIB_ROW), 1, HALF + 1), jax.random.fold_in(streams_of[6], 1), 1, HALF).astype(jnp.int32),
        "owner_slot": draw_owner_slot(jax.random.fold_in(streams_of[8], 71), 0),
    }


def high_dot(first, second):
    return jnp.dot(first, second, precision=lax.Precision.HIGHEST)

def square_roots(gram):
    order = gram.shape[0]
    identity = jnp.eye(order, dtype=jnp.float32)
    scale_value = jnp.sqrt(jnp.sum(gram * gram))
    root_now = gram / scale_value
    inverse_now = identity
    for repeat in range(ROOTS):
        middle = 1.5 * identity - 0.5 * high_dot(inverse_now, root_now)
        root_now = high_dot(root_now, middle)
        inverse_now = high_dot(middle, inverse_now)
    return (root_now * jnp.sqrt(scale_value), inverse_now / jnp.sqrt(scale_value))

def recompress(old_left, old_right, old_rank, add_left, add_right, add_rank, keep_rank):
    half_width = old_left.shape[1]
    column = jnp.arange(2 * half_width)
    live_mask = jnp.where(column < half_width, column < old_rank, column - half_width < add_rank).astype(jnp.float32)
    stack_left = jnp.concatenate([old_left, add_left], axis=1).astype(jnp.float32) * live_mask
    stack_right = jnp.concatenate([old_right, add_right], axis=1).astype(jnp.float32) * live_mask
    gram_left = high_dot(stack_left.T, stack_left)
    gram_right = high_dot(stack_right.T, stack_right) + jnp.diag(1.0 - live_mask)
    root_factor, inverse_factor = square_roots(gram_right)
    core_matrix = high_dot(high_dot(root_factor, gram_left), root_factor)
    subspace = core_matrix[:, :half_width] + core_matrix[:, half_width:]
    subspace = subspace / jnp.sqrt(jnp.sum(subspace * subspace) + 1e-06)
    for repeat in range(SWEEPS):
        inner = high_dot(subspace.T, subspace)
        subspace = 1.5 * subspace - 0.5 * high_dot(subspace, inner)
    subspace_kept = subspace * (jnp.arange(half_width) < keep_rank).astype(jnp.float32)
    new_left = high_dot(stack_left, high_dot(root_factor, subspace_kept))
    solved = high_dot(inverse_factor, subspace_kept)
    new_right = high_dot(stack_right, solved) * math.sqrt(stack_right.shape[0])
    return (new_left.astype(jnp.bfloat16), new_right.astype(jnp.bfloat16))

def reference(current_left, current_right, current_rank, target_rank, update_left, update_right, update_rank, owner_slot):
    row_count = current_rank.shape[0]
    tile_total = current_rank.shape[1]
    flat_tile = (owner_slot + jnp.arange(row_count, dtype=jnp.int32)[:, None] * tile_total).reshape(-1).astype(jnp.int32)
    tile_shape = current_left.shape[2:]
    flat_left = current_left.reshape((-1,) + tile_shape)
    flat_right = current_right.reshape((-1,) + tile_shape)
    items = (jnp.take(flat_left, flat_tile, axis=0), jnp.take(flat_right, flat_tile, axis=0), jnp.take(current_rank.reshape(-1), flat_tile), update_left.reshape((-1,) + tile_shape), update_right.reshape((-1,) + tile_shape), update_rank.reshape(-1), jnp.take(target_rank.reshape(-1), flat_tile))

    def single(entry):
        return recompress(*entry)
    new_left, new_right = lax.map(single, items)
    keep_cols = jnp.arange(HALF) < current_rank[:, :, None]
    masked = jnp.where(keep_cols[:, :, None, :], current_left, jnp.zeros((), current_left.dtype))
    compressed_left = masked.reshape((-1,) + tile_shape).at[flat_tile].set(new_left).reshape(current_left.shape)
    returned_right = new_right.reshape(update_left.shape)
    squares = lax.optimization_barrier(jnp.sum(jnp.square(compressed_left.astype(jnp.float32)), axis=3))
    row_sum = lax.optimization_barrier(jnp.sum(squares.reshape(row_count, tile_total // BR, BR, TILE), axis=1)).reshape(row_count * BR, TILE)
    mean_value = jnp.sum(row_sum) / (row_count * BR * TILE)
    row_scale = jnp.sqrt(row_sum / mean_value)
    return (compressed_left, returned_right, row_scale)
```

```python
import math

import jax
import jax.numpy as jnp
from jax import lax
from jax.experimental import pallas as pl
from jax.experimental.pallas import tpu as pltpu
from jax.sharding import PartitionSpec as P

BR = 2
SWEEPS = 8
ROOTS = 3
TOGETHER = 2
HALFWAY = 4
F32 = jnp.float32
BF16 = jnp.bfloat16
TAIL = 16


def parts_of(value):
    high = value.astype(BF16)
    return high, (value - high.astype(F32)).astype(BF16)


def plain(first, second):
    return jnp.dot(first, second, preferred_element_type=F32)


def over_rows(first, second):
    return lax.dot_general(first, second, (((0,), (0,)), ((), ())), preferred_element_type=F32)


def wide(first, second):
    return plain(first[0], second[0]) + (plain(first[0], second[1]) + plain(first[1], second[0]))


def tall(first, second):
    half = second[0].shape[1]
    both = plain(first[0], jnp.concatenate(second, axis=1))
    return both[:, :half] + (both[:, half:] + plain(first[1], second[0]))


def narrow(first, second):
    half = second[0].shape[1]
    right = jnp.concatenate(second, axis=1)
    both = plain(jnp.concatenate(first, axis=1), jnp.concatenate([right, right], axis=0))
    return both[:, :half] + both[:, half:]


def self_product(value):
    both = jnp.concatenate(value, axis=1)
    half = value[0].shape[1]
    four = over_rows(both, both)
    return (four[:half, :half] + four[half:, half:]) + (four[:half, half:] + four[half:, :half])


def eye(order):
    return (
        lax.broadcasted_iota(jnp.int32, (order, order), 0)
        == lax.broadcasted_iota(jnp.int32, (order, order), 1)
    ).astype(F32)


def total_of(value):
    return jnp.sum(jnp.sum(value, axis=1, keepdims=True), axis=0, keepdims=True)


def recompress_body(meta, own, width, left_in, right_in, add_left, add_right, left_out, right_out):
    half = add_left.shape[2]
    rows = add_left.shape[1]
    piece = left_in.shape[1] // TOGETHER
    tiles_each = width[0]
    lane = lax.broadcasted_iota(jnp.int32, (1, half), 1)
    which = range(TOGETHER)
    ident = eye(2 * half)
    left, right, keep, gram_left, gram_right = [], [], [], [], []
    for n in which:
        spot = pl.program_id(0) * TOGETHER + n
        slot = own[0, spot]
        owner, place = slot // tiles_each, slot % tiles_each
        old_live = (lane < meta[owner, place]).astype(F32)
        add_live = (lane < own[1, spot]).astype(F32)
        keep.append((lane < meta[owner, tiles_each + place]).astype(F32))
        live = jnp.concatenate([old_live, add_live], axis=1)
        narrow_live = live.astype(BF16)

        def stacked(ref, add):
            old = ref[:, n * piece : (n + 1) * piece, :].reshape(rows, half)
            return jnp.concatenate([old, add[n]], axis=1) * narrow_live

        left.append(stacked(left_in, add_left))
        right.append(stacked(right_in, add_right))
        gram_right.append(over_rows(right[n], right[n]) + ident * (1.0 - live))
        gram_left.append(over_rows(left[n], left[n]))
    scale, root, inverse = [], [], []
    for n in which:
        scale.append(jnp.sqrt(total_of(gram_right[n] * gram_right[n])))
        root.append(gram_right[n] / scale[n])
    for n in which:
        middle = 1.5 * ident - 0.5 * root[n]
        cut = parts_of(middle)
        root[n] = wide(parts_of(root[n]), cut)
        inverse.append(middle)
    for repeat in range(1, ROOTS):
        for n in which:
            root_cut, inverse_cut = parts_of(root[n]), parts_of(inverse[n])
            middle = parts_of(1.5 * ident - 0.5 * wide(inverse_cut, root_cut))
            root[n] = wide(root_cut, middle)
            inverse[n] = wide(middle, inverse_cut)
    root = [parts_of(r) for r in root]
    inverse = [parts_of(r) for r in inverse]
    space = []
    for n in which:
        full = root[n][0].astype(F32) + root[n][1].astype(F32)
        folded = parts_of(full[:, :half] + full[:, half:])
        core = tall(root[n], parts_of(tall(parts_of(gram_left[n]), folded))) * scale[n]
        space.append(core / jnp.sqrt(total_of(core * core) + 1e-06))
    ident = eye(half)
    for block in range(SWEEPS // HALFWAY):
        cut = [parts_of(space[n]) for n in which]
        inner = [self_product(cut[n]) for n in which]
        gathered = [None] * TOGETHER
        for repeat in range(HALFWAY):
            for n in which:
                factor = parts_of(1.5 * ident - 0.5 * inner[n])
                if repeat + 1 < HALFWAY:
                    inner[n] = narrow(parts_of(narrow(parts_of(inner[n]), factor)), factor)
                gathered[n] = factor if repeat == 0 else parts_of(narrow(gathered[n], factor))
        space = [narrow(cut[n], gathered[n]) for n in which]
    for n in which:
        kept = parts_of(space[n] * keep[n])
        square_root = jnp.sqrt(scale[n])
        on_left = jnp.concatenate(parts_of(tall(root[n], kept) * square_root), axis=1)
        on_right = jnp.concatenate(parts_of(tall(inverse[n], kept) / square_root), axis=1)
        new_left = plain(left[n], on_left)
        new_left = (new_left[:, :half] + new_left[:, half:]).astype(BF16)
        left_out[:, n * piece : (n + 1) * piece, :] = new_left.reshape(-1, piece, half)
        new_right = plain(right[n], on_right)
        new_right = (new_right[:, :half] + new_right[:, half:]) * math.sqrt(rows)
        right_out[n] = new_right.astype(BF16)


def recompress(meta, own, width, arrived, add_left, add_right):
    peers, span, half = arrived.shape
    slots, rows, _ = add_left.shape
    piece = rows // peers
    steps = slots // TOGETHER
    pieces = (peers, TOGETHER * piece, half)
    whole = (TOGETHER, rows, half)
    return pl.pallas_call(
        recompress_body,
        grid_spec=pltpu.PrefetchScalarGridSpec(
            num_scalar_prefetch=3,
            grid=(steps,),
            in_specs=[
                pl.BlockSpec(pieces, lambda g, *_: (0, g, 0)),
                pl.BlockSpec(pieces, lambda g, *_: (0, g + steps, 0)),
                pl.BlockSpec(whole, lambda g, *_: (g, 0, 0)),
                pl.BlockSpec(whole, lambda g, *_: (g, 0, 0)),
            ],
            out_specs=[
                pl.BlockSpec(pieces, lambda g, *_: (0, g, 0)),
                pl.BlockSpec(whole, lambda g, *_: (g, 0, 0)),
            ],
        ),
        out_shape=[
            jax.ShapeDtypeStruct((peers, slots * piece, half), BF16),
            jax.ShapeDtypeStruct((slots, rows, half), BF16),
        ],
        compiler_params=pltpu.CompilerParams(
            dimension_semantics=("arbitrary",), vmem_limit_bytes=60 * 2**20
        ),
        name="recompress",
    )(meta, own, width, arrived, arrived, add_left, add_right)


def pack_body(left, right, meta, out, done):
    tiles, rows, _ = left.shape
    peers = out.shape[0]
    piece = rows // peers

    def one_peer(peer, carry):
        def one_tile(tile, inner):
            source = pl.ds(pl.multiple_of(peer * piece, TAIL), piece)
            for at, ref in ((0, left), (tiles * piece, right)):
                target = pl.ds(pl.multiple_of(at + tile * piece, TAIL), piece)
                pltpu.make_async_copy(ref.at[tile, source], out.at[peer, target], done).start()
            return inner

        lax.fori_loop(0, tiles, one_tile, 0, unroll=4)
        pltpu.make_async_copy(meta, out.at[peer, pl.ds(2 * tiles * piece, TAIL)], done).start()
        return carry

    lax.fori_loop(0, peers, one_peer, 0)
    pltpu.make_async_copy(out, out, done).wait()


def in_memory():
    return pl.BlockSpec(memory_space=pltpu.HBM)


def pack(left, right, meta, peers):
    tiles, rows, half = left.shape
    span = 2 * tiles * (rows // peers) + TAIL
    return pl.pallas_call(
        pack_body,
        in_specs=[in_memory()] * 3,
        out_specs=in_memory(),
        out_shape=jax.ShapeDtypeStruct((peers, span, half), BF16),
        scratch_shapes=[pltpu.SemaphoreType.DMA],
        name="pack",
    )(left, right, meta)


def pick_body(tiles, meta, pieces, out, named_by, done):
    peers, span, _ = pieces.shape
    piece = (span - TAIL) // (2 * tiles)
    slots = out.shape[1] // (2 * piece)

    def one_peer(peer, carry):
        for s in range(slots):
            slot = meta[peer, 2 * tiles + s]
            owner, place = slot // tiles, slot % tiles
            for at, to in ((0, 0), (tiles * piece, slots * piece)):
                source = pl.ds(pl.multiple_of(at + place * piece, TAIL), piece)
                pltpu.make_async_copy(
                    pieces.at[owner, source], out.at[peer, pl.ds(to + s * piece, piece)], done
                ).start()
        return carry

    lax.fori_loop(0, peers, one_peer, 0)

    def clear(tile, carry):
        named_by[tile] = -1
        return carry

    lax.fori_loop(0, peers * tiles, clear, 0, unroll=8)

    def note(peer, carry):
        for s in range(slots):
            named_by[meta[peer, 2 * tiles + s]] = peer * slots + s
        return carry

    lax.fori_loop(0, peers, note, 0)
    pltpu.make_async_copy(out, out, done).wait()


def pick(meta, pieces, tiles, slots):
    peers, span, half = pieces.shape
    piece = (span - TAIL) // (2 * tiles)

    def body(*refs):
        pick_body(tiles, *refs)

    return pl.pallas_call(
        body,
        in_specs=[pl.BlockSpec(memory_space=pltpu.SMEM), in_memory()],
        out_specs=[in_memory(), pl.BlockSpec(memory_space=pltpu.SMEM)],
        out_shape=[
            jax.ShapeDtypeStruct((peers, 2 * slots * piece, half), BF16),
            jax.ShapeDtypeStruct((peers * tiles,), jnp.int32),
        ],
        scratch_shapes=[pltpu.SemaphoreType.DMA],
        name="pick",
    )(meta, pieces)


def place_body(tiles, meta, named_by, fresh, old, out, sums):
    peers, span, half = fresh.shape
    piece = old.shape[1] // tiles
    slots = span // piece
    lane = lax.broadcasted_iota(jnp.int32, (piece, half), 1)

    def one_owner(owner, totals):
        totals = list(totals)
        for tile in range(tiles):
            who = named_by[owner * tiles + tile]
            safe = jnp.maximum(who, 0)
            at = pl.multiple_of((safe % slots) * piece, TAIL)
            new = fresh[safe // slots, pl.ds(at, piece), :].astype(F32)
            own = old[owner, tile * piece : (tile + 1) * piece, :].astype(F32)
            limit = jnp.where(who < 0, meta[owner, tile], half)
            value = jnp.where(lane < limit, jnp.where(who < 0, own, new), 0.0)
            out[owner, tile * piece : (tile + 1) * piece, :] = value.astype(BF16)
            totals[tile % BR] += value * value
        return tuple(totals)

    totals = lax.fori_loop(
        0, peers, one_owner, tuple(jnp.zeros((piece, half), F32) for _ in range(BR))
    )
    tail_lane = lax.broadcasted_iota(jnp.int32, (TAIL, half), 1)
    tail = jnp.zeros((TAIL, half), F32)
    whole = jnp.zeros((1, 1), F32)
    for k in range(BR):
        row = jnp.sum(totals[k], axis=1, keepdims=True)
        whole += jnp.sum(row, axis=0, keepdims=True)
        for group in range(piece // TAIL):
            rest = row[group * TAIL : (group + 1) * TAIL]
            for part in range(3):
                high = rest.astype(BF16).astype(F32)
                rest = rest - high
                tail = jnp.where(tail_lane == (group * BR + k) * 3 + part, high, tail)
    tail = tail.astype(BF16)
    for peer in range(peers):
        out[peer, tiles * piece :, :] = tail
    sums[...] = jnp.broadcast_to(whole, sums.shape)


def place(meta, named_by, fresh, pieces, tiles):
    peers, span, half = fresh.shape
    piece = (pieces.shape[1] - TAIL) // (2 * tiles)

    def body(*refs):
        place_body(tiles, *refs)

    return pl.pallas_call(
        body,
        grid=(1,),
        in_specs=[
            pl.BlockSpec(memory_space=pltpu.SMEM),
            pl.BlockSpec(memory_space=pltpu.SMEM),
            pl.BlockSpec(fresh.shape, lambda g: (0, 0, 0)),
            pl.BlockSpec((peers, tiles * piece, half), lambda g: (0, 0, 0)),
        ],
        out_specs=[
            pl.BlockSpec((peers, tiles * piece + TAIL, half), lambda g: (0, 0, 0)),
            pl.BlockSpec((8, half), lambda g: (0, 0)),
        ],
        out_shape=[
            jax.ShapeDtypeStruct((peers, tiles * piece + TAIL, half), BF16),
            jax.ShapeDtypeStruct((8, half), F32),
        ],
        compiler_params=pltpu.CompilerParams(vmem_limit_bytes=60 * 2**20),
        name="place",
    )(meta, named_by, fresh, pieces)


def exchange(value, axis):
    return lax.all_to_all(value, axis, split_axis=0, concat_axis=0, tiled=True)


def local(
    current_left,
    current_right,
    current_rank,
    target_rank,
    update_left,
    update_right,
    update_rank,
    owner_slot,
):
    peers = lax.axis_size("col")
    tiles, rows, half = current_left.shape[1:]
    slots = owner_slot.shape[1]
    piece = rows // peers
    table = jnp.concatenate([current_rank, target_rank, owner_slot], axis=1).astype(BF16)
    table = jnp.pad(table, ((0, TAIL - 1), (0, half - table.shape[1])))
    pieces = exchange(pack(current_left[0], current_right[0], table, peers), "col")
    meta = pieces[:, 2 * tiles * piece, :].astype(jnp.int32)
    own = jnp.concatenate([owner_slot, update_rank], axis=0)
    width = jnp.full((1,), tiles, jnp.int32)
    chosen, named_by = pick(meta, pieces, tiles, slots)
    arrived = exchange(chosen, "col")
    fresh, returned_right = recompress(meta, own, width, arrived, update_left[0], update_right[0])
    fresh = exchange(fresh, "col")
    placed, sums = place(meta, named_by, fresh, pieces, tiles)
    placed = exchange(placed, "col")
    kept_left = placed[:, : tiles * piece].reshape(peers, tiles, piece, half)
    kept_left = jnp.swapaxes(kept_left, 0, 1).reshape(tiles, rows, half)
    groups = piece // TAIL
    tail = placed[:, tiles * piece :, : groups * BR * 3].astype(F32)
    tail = jnp.sum(tail.reshape(peers, TAIL, groups, BR, 3), axis=4)
    row_sum = jnp.transpose(tail, (3, 0, 2, 1)).reshape(BR, rows)
    row_total = jnp.broadcast_to(jnp.sum(row_sum), (lax.axis_size("row"), 1, 1))
    front_sum = jnp.sum(exchange(row_total, "row"))
    mean_value = front_sum / (lax.axis_size("row") * BR * rows)
    row_scale = jnp.sqrt(row_sum / mean_value)
    return (kept_left[None], returned_right[None], row_scale)


def solution(mesh):
    return jax.shard_map(
        local,
        mesh=mesh,
        in_specs=(
            P("row", "col", None, None),
            P("row", "col", None, None),
            P("row", "col"),
            P("row", "col"),
            P("row", "col", None, None),
            P("row", "col", None, None),
            P("row", "col"),
            P("row", "col"),
        ),
        out_specs=(P("row", "col", None, None), P("row", "col", None, None), P("row", None)),
        check_vma=False,
    )
```

```python
import math

import jax
import jax.numpy as jnp
from jax import lax
from jax.experimental import pallas as pl
from jax.experimental.pallas import tpu as pltpu
from jax.sharding import PartitionSpec as P

BR = 2
SWEEPS = 8
ROOTS = 3
TOGETHER = 2
HALFWAY = 4
F32 = jnp.float32
BF16 = jnp.bfloat16
TAIL = 16


def parts_of(value):
    high = value.astype(BF16)
    return high, (value - high.astype(F32)).astype(BF16)


def plain(first, second):
    return jnp.dot(first, second, preferred_element_type=F32)


def over_rows(first, second):
    return lax.dot_general(first, second, (((0,), (0,)), ((), ())), preferred_element_type=F32)


def wide(first, second):
    return plain(first[0], second[0]) + (plain(first[0], second[1]) + plain(first[1], second[0]))


def tall(first, second):
    half = second[0].shape[1]
    both = plain(first[0], jnp.concatenate(second, axis=1))
    return both[:, :half] + (both[:, half:] + plain(first[1], second[0]))


def narrow(first, second):
    half = second[0].shape[1]
    right = jnp.concatenate(second, axis=1)
    both = plain(jnp.concatenate(first, axis=1), jnp.concatenate([right, right], axis=0))
    return both[:, :half] + both[:, half:]


def self_product(value):
    both = jnp.concatenate(value, axis=1)
    half = value[0].shape[1]
    four = over_rows(both, both)
    return (four[:half, :half] + four[half:, half:]) + (four[:half, half:] + four[half:, :half])


def eye(order):
    return (
        lax.broadcasted_iota(jnp.int32, (order, order), 0)
        == lax.broadcasted_iota(jnp.int32, (order, order), 1)
    ).astype(F32)


def total_of(value):
    return jnp.sum(jnp.sum(value, axis=1, keepdims=True), axis=0, keepdims=True)


def recompress_step(step, meta, own, width, left_in, right_in, add_left, add_right, left_out, right_out):
    _, rows, half = add_left.shape
    peers = left_in.shape[0]
    piece = rows // peers
    tiles_each = width
    lane = lax.broadcasted_iota(jnp.int32, (1, half), 1)
    which = range(TOGETHER)
    ident = eye(2 * half)
    left, right, keep, gram_left, gram_right = [], [], [], [], []
    for n in which:
        spot = step * TOGETHER + n
        slot = own[0, spot]
        owner, place = slot // tiles_each, slot % tiles_each
        old_live = (lane < meta[owner, place]).astype(F32)
        add_live = (lane < own[1, spot]).astype(F32)
        keep.append((lane < meta[owner, tiles_each + place]).astype(F32))
        live = jnp.concatenate([old_live, add_live], axis=1)
        narrow_live = live.astype(BF16)

        def stacked(ref, at, add):
            old = ref[:, pl.ds(pl.multiple_of(at + spot * piece, TAIL), piece), :]
            return jnp.concatenate([old.reshape(rows, half), add[spot]], axis=1) * narrow_live

        left.append(stacked(left_in, 0, add_left))
        right.append(stacked(right_in, right_in.shape[1] // 2, add_right))
        gram_right.append(over_rows(right[n], right[n]) + ident * (1.0 - live))
        gram_left.append(over_rows(left[n], left[n]))
    scale, root, inverse = [], [], []
    for n in which:
        scale.append(jnp.sqrt(total_of(gram_right[n] * gram_right[n])))
        root.append(gram_right[n] / scale[n])
    for n in which:
        middle = 1.5 * ident - 0.5 * root[n]
        cut = parts_of(middle)
        root[n] = wide(parts_of(root[n]), cut)
        inverse.append(middle)
    for repeat in range(1, ROOTS):
        for n in which:
            root_cut, inverse_cut = parts_of(root[n]), parts_of(inverse[n])
            middle = parts_of(1.5 * ident - 0.5 * wide(inverse_cut, root_cut))
            root[n] = wide(root_cut, middle)
            inverse[n] = wide(middle, inverse_cut)
    root = [parts_of(r) for r in root]
    inverse = [parts_of(r) for r in inverse]
    space = []
    for n in which:
        full = root[n][0].astype(F32) + root[n][1].astype(F32)
        folded = parts_of(full[:, :half] + full[:, half:])
        core = tall(root[n], parts_of(tall(parts_of(gram_left[n]), folded))) * scale[n]
        space.append(core / jnp.sqrt(total_of(core * core) + 1e-06))
    ident = eye(half)
    for block in range(SWEEPS // HALFWAY):
        cut = [parts_of(space[n]) for n in which]
        inner = [self_product(cut[n]) for n in which]
        gathered = [None] * TOGETHER
        for repeat in range(HALFWAY):
            for n in which:
                factor = parts_of(1.5 * ident - 0.5 * inner[n])
                if repeat + 1 < HALFWAY:
                    inner[n] = narrow(parts_of(narrow(parts_of(inner[n]), factor)), factor)
                gathered[n] = factor if repeat == 0 else parts_of(narrow(gathered[n], factor))
        space = [narrow(cut[n], gathered[n]) for n in which]
    for n in which:
        kept = parts_of(space[n] * keep[n])
        square_root = jnp.sqrt(scale[n])
        on_left = jnp.concatenate(parts_of(tall(root[n], kept) * square_root), axis=1)
        on_right = jnp.concatenate(parts_of(tall(inverse[n], kept) / square_root), axis=1)
        new_left = plain(left[n], on_left)
        new_left = (new_left[:, :half] + new_left[:, half:]).astype(BF16)
        spot = step * TOGETHER + n
        left_out[:, pl.ds(pl.multiple_of(spot * piece, TAIL), piece), :] = new_left.reshape(
            peers, piece, half
        )
        new_right = plain(right[n], on_right)
        new_right = (new_right[:, :half] + new_right[:, half:]) * math.sqrt(rows)
        right_out[spot] = new_right.astype(BF16)


def on_chip():
    return pl.BlockSpec(memory_space=pltpu.VMEM)


def scalars():
    return pl.BlockSpec(memory_space=pltpu.SMEM)


def recompress(meta, own, tiles, arrived, add_left, add_right):
    peers, _, half = arrived.shape
    slots, rows, _ = add_left.shape

    def body(meta, own, arrived, add_left, add_right, left_out, right_out):
        def one_step(step, carry):
            recompress_step(
                step, meta, own, tiles, arrived, arrived, add_left, add_right, left_out, right_out
            )
            return carry

        lax.fori_loop(0, slots // TOGETHER, one_step, 0)

    return pl.pallas_call(
        body,
        in_specs=[scalars(), scalars(), on_chip(), on_chip(), on_chip()],
        out_specs=[on_chip(), on_chip()],
        out_shape=[
            jax.ShapeDtypeStruct((peers, slots * (rows // peers), half), BF16),
            jax.ShapeDtypeStruct((slots, rows, half), BF16),
        ],
        compiler_params=pltpu.CompilerParams(vmem_limit_bytes=60 * 2**20),
        name="recompress",
    )(meta, own, arrived, add_left, add_right)


def pack(left, right, rank, target, slot, peers):
    tiles, rows, half = left.shape
    piece = rows // peers
    tail_at = 2 * tiles * piece

    def body(left, right, rank, target, slot, out, table):
        table[...] = jnp.zeros_like(table)
        at = 0
        for ref in (rank, target, slot):
            wide_ref = ref.shape[1]
            table[0:1, at : at + wide_ref] = ref[...]
            at += wide_ref
        tail = table[...].astype(F32).astype(BF16)

        def one_tile(tile, carry):
            for at, ref in ((0, left), (tiles * piece, right)):
                target_rows = pl.ds(pl.multiple_of(at + tile * piece, TAIL), piece)
                out[:, target_rows, :] = ref[tile].reshape(peers, piece, half)
            return carry

        lax.fori_loop(0, tiles, one_tile, 0)
        for peer in range(peers):
            out[peer, tail_at:, :] = tail

    return pl.pallas_call(
        body,
        in_specs=[on_chip()] * 5,
        out_specs=on_chip(),
        out_shape=jax.ShapeDtypeStruct((peers, tail_at + TAIL, half), BF16),
        scratch_shapes=[pltpu.VMEM((TAIL, half), jnp.int32)],
        name="pack",
    )(left, right, rank, target, slot)


def pick(meta, pieces, tiles, slots):
    peers, span, half = pieces.shape
    piece = (span - TAIL) // (2 * tiles)

    def body(meta, pieces, out, named_by):
        def clear(tile, carry):
            named_by[tile] = -1
            return carry

        lax.fori_loop(0, peers * tiles, clear, 0, unroll=8)

        def one_peer(peer, carry):
            for s in range(slots):
                slot = meta[peer, 2 * tiles + s]
                named_by[slot] = peer * slots + s
                owner, place = slot // tiles, slot % tiles
                for at, to in ((0, 0), (tiles * piece, slots * piece)):
                    source = pl.ds(pl.multiple_of(at + place * piece, TAIL), piece)
                    out[peer, to + s * piece : to + (s + 1) * piece, :] = pieces[owner, source, :]
            return carry

        lax.fori_loop(0, peers, one_peer, 0)

    return pl.pallas_call(
        body,
        in_specs=[scalars(), on_chip()],
        out_specs=[on_chip(), scalars()],
        out_shape=[
            jax.ShapeDtypeStruct((peers, 2 * slots * piece, half), BF16),
            jax.ShapeDtypeStruct((peers * tiles,), jnp.int32),
        ],
        name="pick",
    )(meta, pieces)


def place_body(tiles, meta, named_by, fresh, old, out, sums):
    peers, span, half = fresh.shape
    piece = (old.shape[1] - TAIL) // (2 * tiles)
    slots = span // piece
    lane = lax.broadcasted_iota(jnp.int32, (piece, half), 1)

    def one_owner(owner, totals):
        totals = list(totals)
        for tile in range(tiles):
            who = named_by[owner * tiles + tile]
            safe = jnp.maximum(who, 0)
            at = pl.multiple_of((safe % slots) * piece, TAIL)
            new = fresh[safe // slots, pl.ds(at, piece), :].astype(F32)
            own = old[owner, tile * piece : (tile + 1) * piece, :].astype(F32)
            limit = jnp.where(who < 0, meta[owner, tile], half)
            value = jnp.where(lane < limit, jnp.where(who < 0, own, new), 0.0)
            out[owner, tile * piece : (tile + 1) * piece, :] = value.astype(BF16)
            totals[tile % BR] += value * value
        return tuple(totals)

    totals = lax.fori_loop(
        0, peers, one_owner, tuple(jnp.zeros((piece, half), F32) for _ in range(BR))
    )
    tail_lane = lax.broadcasted_iota(jnp.int32, (TAIL, half), 1)
    tail = jnp.zeros((TAIL, half), F32)
    whole = jnp.zeros((1, 1), F32)
    for k in range(BR):
        row = jnp.sum(totals[k], axis=1, keepdims=True)
        whole += jnp.sum(row, axis=0, keepdims=True)
        for group in range(piece // TAIL):
            rest = row[group * TAIL : (group + 1) * TAIL]
            for part in range(3):
                high = rest.astype(BF16).astype(F32)
                rest = rest - high
                tail = jnp.where(tail_lane == (group * BR + k) * 3 + part, high, tail)
    tail = tail.astype(BF16)
    for peer in range(peers):
        out[peer, tiles * piece :, :] = tail
    sums[...] = jnp.broadcast_to(whole, sums.shape)


def place(meta, named_by, fresh, pieces, tiles):
    peers, span, half = fresh.shape
    piece = (pieces.shape[1] - TAIL) // (2 * tiles)

    def body(*refs):
        place_body(tiles, *refs)

    return pl.pallas_call(
        body,
        in_specs=[scalars(), scalars(), on_chip(), on_chip()],
        out_specs=[on_chip(), on_chip()],
        out_shape=[
            jax.ShapeDtypeStruct((peers, tiles * piece + TAIL, half), BF16),
            jax.ShapeDtypeStruct((8, half), F32),
        ],
        name="place",
    )(meta, named_by, fresh, pieces)


def exchange(value, axis):
    return lax.all_to_all(value, axis, split_axis=0, concat_axis=0, tiled=True)


def local(
    current_left,
    current_right,
    current_rank,
    target_rank,
    update_left,
    update_right,
    update_rank,
    owner_slot,
):
    peers = lax.axis_size("col")
    tiles, rows, half = current_left.shape[1:]
    slots = owner_slot.shape[1]
    piece = rows // peers
    packed = pack(
        current_left[0], current_right[0], current_rank, target_rank, owner_slot, peers
    )
    pieces = exchange(packed, "col")
    meta = pieces[:, 2 * tiles * piece, :].astype(jnp.int32)
    own = jnp.concatenate([owner_slot, update_rank], axis=0)
    chosen, named_by = pick(meta, pieces, tiles, slots)
    arrived = exchange(chosen, "col")
    fresh, returned_right = recompress(meta, own, tiles, arrived, update_left[0], update_right[0])
    fresh = exchange(fresh, "col")
    placed, sums = place(meta, named_by, fresh, pieces, tiles)
    placed = exchange(placed, "col")
    kept_left = placed[:, : tiles * piece].reshape(peers, tiles, piece, half)
    kept_left = jnp.swapaxes(kept_left, 0, 1).reshape(tiles, rows, half)
    groups = piece // TAIL
    tail = placed[:, tiles * piece :, : groups * BR * 3].astype(F32)
    tail = jnp.sum(tail.reshape(peers, TAIL, groups, BR, 3), axis=4)
    row_sum = jnp.transpose(tail, (3, 0, 2, 1)).reshape(BR, rows)
    row_total = jnp.broadcast_to(jnp.sum(row_sum), (lax.axis_size("row"), 1, 1))
    front_sum = jnp.sum(exchange(row_total, "row"))
    mean_value = front_sum / (lax.axis_size("row") * BR * rows)
    row_scale = jnp.sqrt(row_sum / mean_value)
    return (kept_left[None], returned_right[None], row_scale)


def solution(mesh):
    return jax.shard_map(
        local,
        mesh=mesh,
        in_specs=(
            P("row", "col", None, None),
            P("row", "col", None, None),
            P("row", "col"),
            P("row", "col"),
            P("row", "col", None, None),
            P("row", "col", None, None),
            P("row", "col"),
            P("row", "col"),
        ),
        out_specs=(P("row", "col", None, None), P("row", "col", None, None), P("row", None)),
        check_vma=False,
    )
```

```python
import math

import jax
import jax.numpy as jnp
from jax import lax
from jax.experimental import pallas as pl
from jax.experimental.pallas import tpu as pltpu
from jax.sharding import PartitionSpec as P

BR = 2
SWEEPS = 8
ROOTS = 3
SPLIT = (4, 4)
HALFWAY = 4
F32 = jnp.float32
BF16 = jnp.bfloat16
TAIL = 16


def parts_of(value):
    high = value.astype(BF16)
    return high, (value - high.astype(F32)).astype(BF16)


def plain(first, second):
    return jnp.dot(first, second, preferred_element_type=F32)


def over_rows(first, second):
    return lax.dot_general(first, second, (((0,), (0,)), ((), ())), preferred_element_type=F32)


def wide(first, second):
    rows = first[0].shape[0]
    top = plain(jnp.concatenate(first, axis=0), second[0])
    return top[:rows] + (top[rows:] + plain(first[0], second[1]))


def tall(first, second):
    rows, half = first[0].shape[0], second[0].shape[1]
    four = plain(jnp.concatenate(first, axis=0), jnp.concatenate(second, axis=1))
    return four[:rows, :half] + ((four[:rows, half:] + four[rows:, :half]) + four[rows:, half:])


def narrow(first, second):
    half = second[0].shape[1]
    right = jnp.concatenate(second, axis=1)
    both = plain(jnp.concatenate(first, axis=1), jnp.concatenate([right, right], axis=0))
    return both[:, :half] + both[:, half:]


def self_product(value):
    both = jnp.concatenate(value, axis=1)
    half = value[0].shape[1]
    four = over_rows(both, both)
    return (four[:half, :half] + four[half:, half:]) + (four[:half, half:] + four[half:, :half])


def eye(order):
    return (
        lax.broadcasted_iota(jnp.int32, (order, order), 0)
        == lax.broadcasted_iota(jnp.int32, (order, order), 1)
    ).astype(F32)


def total_of(value):
    return jnp.sum(jnp.sum(value, axis=1, keepdims=True), axis=0, keepdims=True)


def recompress_part(first, meta, own, tiles_each, arrived, add_left, add_right, left_out, right_out):
    count, rows, half = add_left.shape
    peers = arrived.shape[0]
    piece = rows // peers
    left_in = right_in = arrived
    lane = lax.broadcasted_iota(jnp.int32, (1, half), 1)
    which = range(count)
    ident = eye(2 * half)
    left, right, keep, gram_left, gram_right = [], [], [], [], []
    for n in which:
        spot = first + n
        slot = own[0, spot]
        owner, place = slot // tiles_each, slot % tiles_each
        old_live = (lane < meta[owner, place]).astype(F32)
        add_live = (lane < own[1, spot]).astype(F32)
        keep.append((lane < meta[owner, tiles_each + place]).astype(F32))
        live = jnp.concatenate([old_live, add_live], axis=1)
        narrow_live = live.astype(BF16)

        def stacked(ref, at, add):
            old = ref[:, at + n * piece : at + (n + 1) * piece, :]
            return jnp.concatenate([old.reshape(rows, half), add[n]], axis=1) * narrow_live

        left.append(stacked(left_in, 0, add_left))
        right.append(stacked(right_in, right_in.shape[1] // 2, add_right))
        gram_right.append(over_rows(right[n], right[n]) + ident * (1.0 - live))
        gram_left.append(over_rows(left[n], left[n]))
    scale, root, inverse = [], [], []
    for n in which:
        scale.append(jnp.sqrt(total_of(gram_right[n] * gram_right[n])))
        root.append(gram_right[n] / scale[n])
    for n in which:
        middle = 1.5 * ident - 0.5 * root[n]
        cut = parts_of(middle)
        root[n] = wide(parts_of(root[n]), cut)
        inverse.append(middle)
    for repeat in range(1, ROOTS):
        for n in which:
            root_cut, inverse_cut = parts_of(root[n]), parts_of(inverse[n])
            middle = parts_of(1.5 * ident - 0.5 * wide(inverse_cut, root_cut))
            joined = [jnp.concatenate(p, axis=0) for p in zip(root_cut, inverse_cut)]
            joined = wide(joined, middle)
            root[n], inverse[n] = joined[: 2 * half], joined[2 * half :]
    root = [parts_of(r) for r in root]
    inverse = [parts_of(r) for r in inverse]
    space = []
    for n in which:
        full = root[n][0].astype(F32) + root[n][1].astype(F32)
        folded = parts_of(full[:, :half] + full[:, half:])
        core = tall(root[n], parts_of(tall(parts_of(gram_left[n]), folded))) * scale[n]
        space.append(core / jnp.sqrt(total_of(core * core) + 1e-06))
    ident = eye(half)
    for block in range(SWEEPS // HALFWAY):
        cut = [parts_of(space[n]) for n in which]
        inner = [self_product(cut[n]) for n in which]
        gathered = [None] * count
        for repeat in range(HALFWAY):
            for n in which:
                factor = parts_of(1.5 * ident - 0.5 * inner[n])
                if repeat == 0:
                    gathered[n] = factor
                    once = parts_of(narrow(parts_of(inner[n]), factor))
                    inner[n] = narrow(once, factor)
                elif repeat + 1 < HALFWAY:
                    pair = zip(parts_of(inner[n]), gathered[n])
                    both = narrow([jnp.concatenate(p, axis=0) for p in pair], factor)
                    gathered[n] = parts_of(both[half:])
                    inner[n] = narrow(parts_of(both[:half]), factor)
                else:
                    gathered[n] = parts_of(narrow(gathered[n], factor))
        space = [narrow(cut[n], gathered[n]) for n in which]
    for n in which:
        kept = parts_of(space[n] * keep[n])
        square_root = jnp.sqrt(scale[n])
        pair = zip(root[n], inverse[n])
        small = tall([jnp.concatenate(p, axis=0) for p in pair], kept)
        on_left = jnp.concatenate(parts_of(small[: 2 * half] * square_root), axis=1)
        on_right = jnp.concatenate(parts_of(small[2 * half :] / square_root), axis=1)
        new_left = plain(left[n], on_left)
        new_left = (new_left[:, :half] + new_left[:, half:]).astype(BF16)
        left_out[:, n * piece : (n + 1) * piece, :] = new_left.reshape(peers, piece, half)
        new_right = plain(right[n], on_right)
        new_right = (new_right[:, :half] + new_right[:, half:]) * math.sqrt(rows)
        right_out[n] = new_right.astype(BF16)


def on_chip():
    return pl.BlockSpec(memory_space=pltpu.VMEM)


def scalars():
    return pl.BlockSpec(memory_space=pltpu.SMEM)


def in_memory():
    return pl.BlockSpec(memory_space=pltpu.HBM)


def held(value):
    return pltpu.with_memory_space_constraint(value, pltpu.VMEM)


def outside(value):
    return pltpu.with_memory_space_constraint(value, pltpu.HBM)


def recompress(first, count, meta, own, tiles, arrived, add_left, add_right, before=None):
    peers, _, half = arrived.shape
    slots, rows, _ = add_left.shape

    def body(meta, own, arrived, all_left, all_right, *rest):
        left_out, right_out, add_left, add_right, right_made, fetched, done = rest[-7:]
        ours = pl.ds(first, count)
        fetches = [
            pltpu.make_async_copy(all_right.at[ours], add_right, fetched.at[0]),
            pltpu.make_async_copy(all_left.at[ours], add_left, fetched.at[1]),
        ]
        for fetch in fetches:
            fetch.start()
        for fetch in fetches:
            fetch.wait()
        recompress_part(
            first, meta, own, tiles, arrived, add_left, add_right, left_out, right_made
        )
        saved = pltpu.make_async_copy(right_made, right_out.at[pl.ds(first, count)], done)
        saved.start()
        saved.wait()

    operands = [meta, own, held(arrived), outside(add_left), outside(add_right)]
    specs = [scalars(), scalars(), on_chip(), in_memory(), in_memory()]
    if before is not None:
        operands.append(outside(before))
        specs.append(in_memory())
    return pl.pallas_call(
        body,
        in_specs=specs,
        out_specs=[on_chip(), in_memory()],
        out_shape=[
            pltpu.VMEM((peers, count * (rows // peers), half), BF16),
            pltpu.HBM((slots, rows, half), BF16),
        ],
        scratch_shapes=[pltpu.VMEM((count, rows, half), BF16)] * 3
        + [pltpu.SemaphoreType.DMA((2,)), pltpu.SemaphoreType.DMA],
        input_output_aliases={} if before is None else {5: 1},
        compiler_params=pltpu.CompilerParams(vmem_limit_bytes=32 * 2**20),
        cost_estimate=pl.CostEstimate(
            flops=count * 2**31, transcendentals=0, bytes_accessed=count * 6 * rows * half * 2
        ),
        name="recompress",
    )(*operands)


def pack(left, right, rank, target, slot, peers):
    tiles, rows, half = left.shape
    piece = rows // peers
    tail_at = 2 * tiles * piece

    def body(left, right, rank, target, slot, out, left_here, right_here, done):
        def fetches(tile):
            return [
                pltpu.make_async_copy(left.at[tile], left_here.at[tile], done.at[0, tile]),
                pltpu.make_async_copy(right.at[tile], right_here.at[tile], done.at[1, tile]),
            ]

        for tile in range(tiles):
            for fetch in fetches(tile):
                fetch.start()
        lane = lax.broadcasted_iota(jnp.int32, (TAIL, half), 1)
        table = jnp.zeros((TAIL, half), jnp.int32)
        at = 0
        for ref in (rank, target, slot):
            for k in range(ref.shape[1]):
                table = jnp.where(lane == at, ref[0, k], table)
                at += 1
        table = table.astype(F32).astype(BF16)
        for peer in range(peers):
            out[peer, tail_at:, :] = table
        for tile in range(tiles):
            for at, ref, fetch in zip(
                (0, tiles * piece), (left_here, right_here), fetches(tile), strict=True
            ):
                fetch.wait()
                here = at + tile * piece
                out[:, here : here + piece, :] = ref[tile].reshape(peers, piece, half)

    return pl.pallas_call(
        body,
        in_specs=[in_memory()] * 2 + [scalars()] * 3,
        out_specs=on_chip(),
        out_shape=pltpu.VMEM((peers, tail_at + TAIL, half), BF16),
        scratch_shapes=[
            pltpu.VMEM((tiles, rows, half), BF16),
            pltpu.VMEM((tiles, rows, half), BF16),
            pltpu.SemaphoreType.DMA((2, tiles)),
        ],
        compiler_params=pltpu.CompilerParams(vmem_limit_bytes=20 * 2**20),
        name="pack",
    )(outside(left), outside(right), rank, target, slot)


def pick(meta, pieces, tiles, slots):
    peers, span, half = pieces.shape
    piece = (span - TAIL) // (2 * tiles)
    parts = len(SPLIT)

    def body(meta, pieces, *rest):
        outs, named_by = rest[:parts], rest[parts]

        def clear(tile, carry):
            named_by[tile] = -1
            return carry

        lax.fori_loop(0, peers * tiles, clear, 0, unroll=8)

        def one_peer(peer, carry):
            for s in range(slots):
                slot = meta[peer, 2 * tiles + s]
                named_by[slot] = peer * slots + s
                owner, place = slot // tiles, slot % tiles
                part = 0 if s < SPLIT[0] else 1
                out, spot = outs[part], s - part * SPLIT[0]
                for at, to in ((0, 0), (tiles * piece, SPLIT[part] * piece)):
                    source = pl.ds(pl.multiple_of(at + place * piece, TAIL), piece)
                    target = to + spot * piece
                    out[peer, target : target + piece, :] = pieces[owner, source, :]
            return carry

        lax.fori_loop(0, peers, one_peer, 0)

    return pl.pallas_call(
        body,
        in_specs=[scalars(), on_chip()],
        out_specs=[on_chip()] * parts + [scalars()],
        out_shape=[pltpu.VMEM((peers, 2 * count * piece, half), BF16) for count in SPLIT]
        + [jax.ShapeDtypeStruct((peers * tiles,), jnp.int32)],
        compiler_params=pltpu.CompilerParams(vmem_limit_bytes=8 * 2**20),
        name="pick",
    )(meta, held(pieces))


def place_early(meta, named_by, fresh, pieces, tiles):
    peers, _, half = pieces.shape
    piece = (pieces.shape[1] - TAIL) // (2 * tiles)
    slots = sum(SPLIT)

    def body(meta, named_by, fresh, pieces, out, sums, old, fetched):
        fetch = pltpu.make_async_copy(pieces.at[:, pl.ds(0, tiles * piece)], old, fetched)
        fetch.start()
        fetch.wait()
        lane = lax.broadcasted_iota(jnp.int32, (piece, half), 1)

        def one_owner(owner, totals):
            totals = list(totals)
            for tile in range(tiles):
                who = named_by[owner * tiles + tile]
                safe = jnp.maximum(who, 0)
                spot = safe % slots
                at = jnp.minimum(spot, SPLIT[0] - 1) * piece
                new = fresh[safe // slots, pl.ds(pl.multiple_of(at, TAIL), piece), :].astype(F32)
                own = old[owner, tile * piece : (tile + 1) * piece, :].astype(F32)
                limit = jnp.where(spot < SPLIT[0], half, 0)
                limit = jnp.where(who < 0, meta[owner, tile], limit)
                value = jnp.where(lane < limit, jnp.where(who < 0, own, new), 0.0)
                out[owner, tile * piece : (tile + 1) * piece, :] = value.astype(BF16)
                totals[tile % BR] += value * value
            return tuple(totals)

        totals = lax.fori_loop(
            0, peers, one_owner, tuple(jnp.zeros((piece, half), F32) for _ in range(BR))
        )
        for k in range(BR):
            sums[k] = totals[k]

    return pl.pallas_call(
        body,
        in_specs=[scalars(), scalars(), on_chip(), in_memory()],
        out_specs=[on_chip(), on_chip()],
        out_shape=[
            pltpu.VMEM((peers, tiles * piece + TAIL, half), BF16),
            pltpu.VMEM((BR, piece, half), F32),
        ],
        scratch_shapes=[
            pltpu.VMEM((peers, tiles * piece, half), BF16),
            pltpu.SemaphoreType.DMA,
        ],
        compiler_params=pltpu.CompilerParams(vmem_limit_bytes=12 * 2**20),
        cost_estimate=pl.CostEstimate(flops=2**32, transcendentals=0, bytes_accessed=2**23),
        name="place_early",
    )(meta, named_by, held(fresh), outside(pieces))


def three_parts(value):
    parts = []
    for _ in range(3):
        parts.append(value.astype(BF16))
        value = value - parts[-1].astype(F32)
    return parts


def place_late(meta, fresh, placed, sums, tiles):
    peers, span, half = placed.shape
    piece = (span - TAIL) // tiles

    def body(meta, fresh, before, sums, out, whole):
        def one_peer(peer, totals):
            totals = list(totals)
            for n in range(SPLIT[1]):
                slot = meta[peer, 2 * tiles + SPLIT[0] + n]
                owner, tile = slot // tiles, slot % tiles
                value = fresh[peer, n * piece : (n + 1) * piece, :]
                out[owner, pl.ds(pl.multiple_of(tile * piece, TAIL), piece), :] = value
                square = jnp.square(value.astype(F32))
                for k in range(BR):
                    totals[k] += jnp.where(tile % BR == k, square, 0.0)
            return tuple(totals)

        totals = lax.fori_loop(0, peers, one_peer, tuple(sums[k] for k in range(BR)))
        row = lax.broadcasted_iota(jnp.int32, (TAIL, half), 0)
        tail = jnp.zeros((TAIL, half), F32)
        total = jnp.zeros((1, 1), F32)
        ones = jnp.ones((TAIL, half), BF16)
        spare = jnp.zeros((half - piece, half), F32)
        for k in range(BR):
            along = jnp.zeros((TAIL, half), F32)
            for part in three_parts(jnp.concatenate([totals[k], spare], axis=0)):
                along += lax.dot_general(
                    ones, part, (((1,), (1,)), ((), ())), preferred_element_type=F32
                )
            total += jnp.sum(along[0:1], axis=1, keepdims=True)
            for at, part in enumerate(three_parts(along)):
                tail = jnp.where(row == k * 3 + at, part.astype(F32), tail)
        tail = tail.astype(BF16)
        for peer in range(peers):
            out[peer, tiles * piece :, :] = tail
        whole[...] = jnp.broadcast_to(total, whole.shape)

    return pl.pallas_call(
        body,
        in_specs=[scalars(), on_chip(), on_chip(), on_chip()],
        out_specs=[on_chip(), on_chip()],
        out_shape=[pltpu.VMEM(placed.shape, BF16), jax.ShapeDtypeStruct((1, half), F32)],
        input_output_aliases={2: 0},
        compiler_params=pltpu.CompilerParams(vmem_limit_bytes=4 * 2**20),
        name="place_late",
    )(meta, held(fresh), held(placed), held(sums))


def finish(placed, front_sum, tiles, entries):
    peers, span, half = placed.shape
    piece = (span - TAIL) // tiles

    def body(placed, front_sum, out, scale, done):
        saves = [
            pltpu.make_async_copy(
                placed.at[:, pl.ds(tile * piece, piece)], out.at[tile], done.at[tile]
            )
            for tile in range(tiles)
        ]
        for save in saves:
            save.start()
        mean = front_sum[...] / entries
        for peer in range(peers):
            tail = placed[peer, tiles * piece :, :].astype(F32)
            for k in range(BR):
                row = tail[3 * k : 3 * k + 1] + (tail[3 * k + 1 : 3 * k + 2] + tail[3 * k + 2 : 3 * k + 3])
                here = jnp.sqrt(row / mean)
                scale[k : k + 1, peer * piece : (peer + 1) * piece] = here[:, :piece]
        for save in saves:
            save.wait()

    kept, scale = pl.pallas_call(
        body,
        in_specs=[on_chip(), on_chip()],
        out_specs=[in_memory(), on_chip()],
        out_shape=[
            pltpu.HBM((tiles, peers, piece, half), BF16),
            jax.ShapeDtypeStruct((BR, peers * piece), F32),
        ],
        scratch_shapes=[pltpu.SemaphoreType.DMA((tiles,))],
        compiler_params=pltpu.CompilerParams(vmem_limit_bytes=4 * 2**20),
        name="finish",
    )(held(placed), front_sum)
    return kept.reshape(tiles, peers * piece, half), scale


def exchange(value, axis):
    return lax.all_to_all(value, axis, split_axis=0, concat_axis=0, tiled=True)


def sum_over(value, axis, digits):
    size = lax.axis_size(axis)
    stride = size
    for digit in digits:
        stride //= digit
        own = value
        for shift in range(1, digit):
            pairs = []
            for source in range(size):
                place = source // stride % digit
                target = source + ((place + shift) % digit - place) * stride
                pairs.append((source, target))
            value = value + lax.ppermute(own, axis, pairs)
    return value


def local(
    current_left,
    current_right,
    current_rank,
    target_rank,
    update_left,
    update_right,
    update_rank,
    owner_slot,
):
    peers = lax.axis_size("col")
    tiles, rows, half = current_left.shape[1:]
    slots = owner_slot.shape[1]
    piece = rows // peers
    packed = pack(
        current_left[0], current_right[0], current_rank, target_rank, owner_slot, peers
    )
    pieces = exchange(packed, "col")
    meta = pieces[:, 2 * tiles * piece, :].astype(jnp.int32)
    own = jnp.concatenate([owner_slot, update_rank], axis=0)
    *chosen, named_by = pick(meta, pieces, tiles, slots)
    returned_right, fresh = None, []
    for part, value in enumerate(chosen):
        arrived = exchange(value, "col")
        new_left, returned_right = recompress(
            part * SPLIT[0],
            SPLIT[part],
            meta,
            own,
            tiles,
            arrived,
            update_left[0],
            update_right[0],
            returned_right,
        )
        fresh.append(exchange(new_left, "col"))
    placed, sums = place_early(meta, named_by, fresh[0], pieces, tiles)
    placed, whole = place_late(meta, fresh[1], placed, sums, tiles)
    placed = exchange(placed, "col")
    front_sum = sum_over(sum_over(whole, "row", (4, 2)), "col", (16,))
    entries = lax.axis_size("row") * BR * rows
    kept_left, row_scale = finish(placed, front_sum, tiles, entries)
    return (kept_left[None], returned_right[None], row_scale)


def solution(mesh):
    return jax.shard_map(
        local,
        mesh=mesh,
        in_specs=(
            P("row", "col", None, None),
            P("row", "col", None, None),
            P("row", "col"),
            P("row", "col"),
            P("row", "col", None, None),
            P("row", "col", None, None),
            P("row", "col"),
            P("row", "col"),
        ),
        out_specs=(P("row", "col", None, None), P("row", "col", None, None), P("row", None)),
        check_vma=False,
    )
```
